32 devices in a mesh: dom: 8 (over z, x), feat: 4 (over y, core).
Axes of the slice: x: 2, y: 2, z: 4, core: 2. Of those that a mesh axis runs over, the one named last changes fastest.
Arguments:
- items: bfloat16 [2048, 1024], P('dom', 'feat'), may hold values from -6 to 6
- self_ids: int32 [2048], P('dom'), may hold values from 0 to 2047
- neighbor_ids: int32 [2048, 50], P('dom'), may hold values from 0 to 2047
- visit_counts: int32 [2048, 50], P('dom'), may hold values from 1 to 63
- w_self: bfloat16 [1024, 1024], P('feat'), may hold values from -0.1875 to 0.1875
- w_neighbor: bfloat16 [1024, 1024], P('feat'), may hold values from -0.75 to 0.75
- bias: float32 [1024], replicated, may hold values from -3 to 3
Outputs:
- embedding: float32 [2048, 1024], P('dom', 'feat')
The draws below stay inside these ranges and needn't reach their ends.
All inputs are finite; a program needn't handle non-finite values.
Results may differ from the reference program's by a relative error of at most 0.0018.
Values may be sent and summed in bfloat16 or wider, within the bound.
A program may use at most 64 MiB of HBM per device.

```python
import jax
import jax.numpy as jnp
from jax import lax

F = 1024
OUT = 1024
NBR = 50
ITEMS = 2048
BATCH = 2048


def set_ends(values, stream_key, low, high):
    longest = values.shape.index(max(values.shape))
    spots = []
    for shift in (0, 1):
        where = [jax.random.randint(jax.random.fold_in(stream_key, axis), (), 0, length) for axis, length in enumerate(values.shape)]
        where[longest] = (where[longest] + shift) % values.shape[longest]
        spots.append(tuple(where))
    return values.at[spots[0]].set(low).at[spots[1]].set(high)


def block_levels(own_key, dims, pieces, smallest, largest):
    factor_of, own = 1.0, jax.random.fold_in(own_key, 6)
    for axis_at, shards_of in pieces:
        steps = jnp.exp(jax.random.uniform(jax.random.fold_in(own, axis_at), (shards_of,), jnp.float32, smallest / len(pieces), largest / len(pieces)))
        factor_of = factor_of * jnp.repeat(steps, dims[axis_at] // shards_of).reshape([-1 if axis == axis_at else 1 for axis in range(len(dims))])
    return factor_of


def bell_draw(stream_key, dims, width, limit, pieces=(), held_as=jnp.bfloat16):
    drawn = width * jax.random.normal(stream_key, dims, jnp.float32)
    if pieces:
        drawn = drawn * block_levels(stream_key, dims, pieces, -0.22, 0.18)
    return jnp.clip(drawn, -limit, limit).astype(held_as)


def setup_inputs(seed: int = 0) -> dict:
    key_of = jax.random.split(jax.random.key(seed), 8)
    return {
        "items": bell_draw(key_of[0], (ITEMS, F), 1.0, 6.0, ((0, 8), (1, 4))),
        "self_ids": set_ends(jax.random.randint(key_of[1], (BATCH,), 0, ITEMS), jax.random.fold_in(key_of[1], 1), 0, ITEMS - 1).astype(jnp.int32),
        "neighbor_ids": set_ends(jax.random.randint(key_of[2], (BATCH, NBR), 0, ITEMS), jax.random.fold_in(key_of[2], 1), 0, ITEMS - 1).astype(jnp.int32),
        "visit_counts": set_ends(jax.random.randint(key_of[3], (BATCH, NBR), 1, 64), jax.random.fold_in(key_of[3], 1), 1, 63).astype(jnp.int32),
        "w_self": bell_draw(key_of[4], (F, OUT), F ** -0.5, 0.1875, ((0, 4),)),
        "w_neighbor": bell_draw(key_of[5], (F, OUT), (F // 16) ** -0.5, 0.75, ((0, 4),)),
        "bias": bell_draw(key_of[6], (OUT,), 0.5, 3.0, (), jnp.float32),
    }


def reference(items, self_ids, neighbor_ids, visit_counts, w_self, w_neighbor, bias):
    own = items[self_ids]
    total = lax.optimization_barrier(jnp.sum(visit_counts.astype(jnp.float32), axis=1))
    block = 512 if BATCH % 512 == 0 else BATCH
    ids_blocks = neighbor_ids.reshape(BATCH // block, block, NBR)
    count_blocks = visit_counts.reshape(BATCH // block, block, NBR)

    def pool(pair):
        ids, counts = pair
        rows = items[ids].astype(jnp.float32)
        return jnp.einsum('bk,bkf->bf', counts.astype(jnp.float32), rows)
    sums = lax.map(pool, (ids_blocks, count_blocks)).reshape(BATCH, F)
    pooled = (sums / total[:, None]).astype(jnp.bfloat16)
    pre = jnp.dot(own, w_self, preferred_element_type=jnp.float32) + jnp.dot(pooled, w_neighbor, preferred_element_type=jnp.float32)
    hidden = jnp.maximum(pre + bias[None, :], 0.0)
    scale = jnp.sqrt(lax.optimization_barrier(jnp.mean(hidden * hidden, axis=1, keepdims=True)) + 1e-06)
    return hidden / scale
```

```python
import functools

import jax
import jax.numpy as jnp
from jax import lax
from jax.experimental import pallas as pl
from jax.experimental.pallas import tpu as pltpu
from jax.sharding import PartitionSpec as P

MESH = pl.DeviceIdType.MESH
LANES = 128
GROUP = 8
PARTS = 2


def kernel(
    D, F,
    items_hbm, self_hbm, ids_hbm, cnt_hbm, ws_hbm, wn_hbm, bias_hbm,
    out_ref,
    items, selfs, ids_t, cnt_t, ws, wn, bias,
    ids, cnt, key_s, lo_s, wgt_s, weights, gathered, acc,
    send_a, recv_a, send_b, recv_b, sq_out, sq_in,
    local_sem,
    up_send, up_recv, down_send, down_recv, x_send, x_recv,
    a_send_sem, a_recv_sem, b_send_sem, b_recv_sem, q_send_sem, q_recv_sem,
):
    dom, feat = lax.axis_index("dom"), lax.axis_index("feat")
    Z, H = D // 2, F // 2
    z, x = dom // 2, lax.rem(dom, 2)
    y, c = feat // 2, lax.rem(feat, 2)
    R, FC = items.shape
    nb = selfs.shape[1]
    nbr = ids.shape[1]
    share = out_ref.shape[1]
    slot = key_s.shape[1] // GROUP
    n_hi = D * R // LANES
    part = R // PARTS

    pairs = ((items_hbm, items), (ids_hbm, ids_t), (cnt_hbm, cnt_t), (self_hbm, selfs), (ws_hbm, ws), (wn_hbm, wn), (bias_hbm, bias))
    local = [pltpu.make_async_copy(a, b, local_sem.at[i]) for i, (a, b) in enumerate(pairs)]
    for copy in local:
        copy.start()

    barrier = pltpu.get_barrier_semaphore()

    def greet(d, f):
        pl.semaphore_signal(barrier, inc=1, device_id=(d, f), device_id_type=MESH)

    greet(dom + 1 - 2 * x, feat)

    @pl.when(z > 0)
    def _():
        greet(dom - 2, feat)

    @pl.when(z < Z - 1)
    def _():
        greet(dom + 2, feat)

    for k in range(1, F):
        greet(dom, lax.rem(feat + k, F))

    pl.semaphore_wait(barrier, F + (z > 0).astype(jnp.int32) + (z < Z - 1).astype(jnp.int32))
    local[0].wait()

    def rows_of(block, h):
        return pl.ds(pl.multiple_of(block * R + h * part, part), part)

    def block_copy(block, h, own, send_sem, recv_sem, target):
        dst = gathered.at[rows_of(block, h), :]
        src = items.at[pl.ds(h * part, part), :] if own else dst
        return pltpu.make_async_remote_copy(
            src_ref=src, dst_ref=dst, send_sem=send_sem, recv_sem=recv_sem,
            device_id=(target, feat), device_id_type=MESH,
        )

    def up_copy(s, h):
        i = s * PARTS + h
        return block_copy(dom - 2 * s, h, s == 0, up_send.at[i], up_recv.at[i], dom + 2)

    def down_copy(s, h):
        i = s * PARTS + h
        return block_copy(dom + 2 * s, h, s == 0, down_send.at[i], down_recv.at[i], dom - 2)

    def x_copy(step, h):
        i = (step + Z - 1) * PARTS + h
        return block_copy(dom + 2 * step, h, step == 0, x_send.at[i], x_recv.at[i], dom + 1 - 2 * x)

    def up_arrived(s, h):
        i = s * PARTS + h
        block_copy(dom - 2 * (s + 1), h, False, up_send.at[i], up_recv.at[i], dom).wait_recv()

    def down_arrived(s, h):
        i = s * PARTS + h
        block_copy(dom + 2 * (s + 1), h, False, down_send.at[i], down_recv.at[i], dom).wait_recv()

    def x_arrived(step, h):
        i = (step + Z - 1) * PARTS + h
        block_copy(dom + 1 - 2 * x + 2 * step, h, False, x_send.at[i], x_recv.at[i], dom).wait_recv()

    for h in range(PARTS):
        @pl.when(z < Z - 1)
        def _():
            up_copy(0, h).start()

        @pl.when(z > 0)
        def _():
            down_copy(0, h).start()

        x_copy(0, h).start()

    def forward(s, h):
        @pl.when(z > s)
        def _():
            up_arrived(s, h)

            @pl.when(z < Z - 1)
            def _():
                up_copy(s + 1, h).start()

            x_copy(-(s + 1), h).start()

        @pl.when(z < Z - 1 - s)
        def _():
            down_arrived(s, h)

            @pl.when(z > 0)
            def _():
                down_copy(s + 1, h).start()

            x_copy(s + 1, h).start()

    for copy in local[1:4]:
        copy.wait()
    ids[...] = jnp.transpose(ids_t[...])
    cnt[...] = jnp.transpose(cnt_t[...])
    wgt_s[...] = jnp.zeros_like(wgt_s)
    lo_s[...] = jnp.zeros_like(lo_s)
    key_s[...] = jnp.zeros_like(key_s)
    for j in range(GROUP):
        ids_j = ids[pl.ds(j, nb // GROUP, stride=GROUP), :]
        at = slice(j * slot, j * slot + nbr)
        key_s[:, at] = (ids_j // LANES) * GROUP + j
        lo_s[:, at] = lax.rem(ids_j, LANES)
        wgt_s[:, at] = cnt[pl.ds(j, nb // GROUP, stride=GROUP), :].astype(jnp.float32)

    K = key_s.shape[1]

    def half_group(g):
        key = key_s[pl.ds(g, 1), :]
        low = lo_s[pl.ds(g, 1), :]
        wgt = wgt_s[pl.ds(g, 1), :]
        left = jnp.where(lax.broadcasted_iota(jnp.int32, (n_hi * GROUP, K), 0) == key, wgt, 0.0)
        right = jnp.where(lax.broadcasted_iota(jnp.int32, (LANES, K), 0) == low, 1.0, 0.0)
        return lax.dot_general(
            left.astype(jnp.bfloat16), right.astype(jnp.bfloat16),
            (((1,), (1,)), ((), ())), preferred_element_type=jnp.float32,
        )

    def build(it, carry):
        first, second = half_group(it * 2), half_group(it * 2 + 1)
        at = pl.ds(pl.multiple_of(nb + it * 2 * GROUP, 2 * GROUP), 2 * GROUP)
        for hi in range(n_hi):
            rows = slice(hi * GROUP, (hi + 1) * GROUP)
            tile = jnp.concatenate([first[rows], second[rows]], axis=0)
            weights[at, hi * LANES:(hi + 1) * LANES] = tile.astype(jnp.bfloat16)
        return carry

    groups = nb // (2 * GROUP)
    lax.fori_loop(0, groups // 2, build, 0)
    forward(0, 0)
    lax.fori_loop(groups // 2, groups, build, 0)
    forward(0, 1)
    self_col = jnp.transpose(jnp.broadcast_to(selfs[...], (LANES, nb)))
    lane = lax.broadcasted_iota(jnp.int32, (nb, LANES), 1)
    for hi in range(n_hi):
        hit = jnp.where(self_col == lane + hi * LANES, 1.0, 0.0)
        weights[0:nb, hi * LANES:(hi + 1) * LANES] = hit.astype(jnp.bfloat16)
    total = jnp.sum(cnt[...].astype(jnp.float32), axis=1, keepdims=True)

    def columns(block):
        return weights[:, pl.ds(pl.multiple_of(block * R, R), R)]

    def add(block):
        rows = pl.ds(pl.multiple_of(block * R, R), R)
        acc[...] += jnp.dot(columns(block), gathered[rows, :], preferred_element_type=jnp.float32)

    def add_line(step, z_now, wait):
        @pl.when((z_now + step >= 0) & (z_now + step < Z))
        def _():
            if wait:
                for h in range(PARTS):
                    x_arrived(step, h)
                add(dom + 1 - 2 * x + 2 * step)
            else:
                add(dom + 2 * step)

    acc[...] = jnp.dot(columns(dom), items[...], preferred_element_type=jnp.float32)
    add_line(0, z, True)
    for s in range(Z - 1):
        if s > 0:
            for h in range(PARTS):
                forward(s, h)
        for step in (-(s + 1), s + 1):
            add_line(step, z, False)
        if s > 0:
            for step in (-s, s):
                add_line(step, z, True)
    for step in (-(Z - 1), Z - 1):
        add_line(step, z, True)

    own = acc[0:nb, :].astype(jnp.bfloat16)
    pooled = (acc[nb:2 * nb, :] / total).astype(jnp.bfloat16)
    local[4].wait()
    local[5].wait()
    local[6].wait()

    def project(yy, cc):
        cols = pl.ds(pl.multiple_of((yy * 2 + cc) * share, share), share)
        return jnp.dot(own, ws[:, cols], preferred_element_type=jnp.float32) + jnp.dot(
            pooled, wn[:, cols], preferred_element_type=jnp.float32
        )

    def a_copy(k):
        return pltpu.make_async_remote_copy(
            src_ref=send_a.at[k], dst_ref=recv_a.at[k], send_sem=a_send_sem.at[k], recv_sem=a_recv_sem.at[k],
            device_id=(dom, feat + 1 - 2 * c), device_id_type=MESH,
        )

    def b_copy(k):
        return pltpu.make_async_remote_copy(
            src_ref=send_b.at[k], dst_ref=recv_b.at[k], send_sem=b_send_sem.at[k], recv_sem=b_recv_sem.at[k],
            device_id=(dom, lax.rem(y + k + 1, H) * 2 + c), device_id_type=MESH,
        )

    for k in range(H):
        send_a[k] = project(lax.rem(y + k + 1, H), 1 - c)
        a_copy(k).start()
    mine = None
    for k in range(H):
        here = project(lax.rem(y + k + 1, H), c)
        a_copy(k).wait_recv()
        summed = here + recv_a[k]
        if k < H - 1:
            send_b[k] = summed.astype(jnp.bfloat16)
            b_copy(k).start()
        else:
            mine = summed + bias[:, pl.ds(pl.multiple_of(feat * share, share), share)]
    for k in range(H - 1):
        b_copy(k).wait_recv()
        mine = mine + recv_b[k].astype(jnp.float32)
    hidden = jnp.maximum(mine, 0.0)
    squares = jnp.sum(hidden * hidden, axis=1, keepdims=True)
    row = jnp.transpose(jnp.broadcast_to(squares, (nb, LANES)))[0:GROUP, :]
    sq_out[...] = row

    def q_copy(k):
        return pltpu.make_async_remote_copy(
            src_ref=sq_out, dst_ref=sq_in.at[k - 1], send_sem=q_send_sem.at[k - 1], recv_sem=q_recv_sem.at[k - 1],
            device_id=(dom, lax.rem(feat + k, F)), device_id_type=MESH,
        )

    for k in range(1, F):
        q_copy(k).start()
    for k in range(1, F):
        q_copy(k).wait_recv()
        row = row + sq_in[k - 1]
    scale = lax.rsqrt(row / (share * F) + 1e-06)[0:1, :]
    column = jnp.transpose(jnp.broadcast_to(scale, (LANES, nb)))
    for i in range(share // LANES):
        at = slice(i * LANES, (i + 1) * LANES)
        out_ref[:, at] = hidden[:, at] * column

    for s in range(Z - 1):
        for h in range(PARTS):
            @pl.when((z < Z - 1) & (z >= s))
            def _():
                up_copy(s, h).wait_send()

            @pl.when((z > 0) & (z < Z - s))
            def _():
                down_copy(s, h).wait_send()
    for step in range(-(Z - 1), Z):
        @pl.when((z + step >= 0) & (z + step < Z))
        def _():
            for h in range(PARTS):
                x_copy(step, h).wait_send()
    for k in range(H):
        a_copy(k).wait_send()
    for k in range(H - 1):
        b_copy(k).wait_send()
    for k in range(1, F):
        q_copy(k).wait_send()


def shards(D, F, items, self_ids, neighbor_ids, visit_counts, w_self, w_neighbor, bias):
    R, FC = items.shape
    nb, nbr = neighbor_ids.shape
    out = bias.shape[0]
    share = out // F
    slot = 1 << (nbr - 1).bit_length()
    Z, H = D // 2, F // 2
    lines = (Z - 1) * PARTS
    f32, bf16, i32 = jnp.float32, jnp.bfloat16, jnp.int32
    dma = pltpu.SemaphoreType.DMA
    return pl.pallas_call(
        functools.partial(kernel, D, F),
        out_shape=jax.ShapeDtypeStruct((nb, share), f32),
        in_specs=[pl.BlockSpec(memory_space=pl.ANY)] * 7,
        out_specs=pl.BlockSpec(memory_space=pltpu.VMEM),
        scratch_shapes=[
            pltpu.VMEM((R, FC), bf16),
            pltpu.VMEM((1, nb), i32),
            pltpu.VMEM((nbr, nb), i32),
            pltpu.VMEM((nbr, nb), i32),
            pltpu.VMEM((FC, out), bf16),
            pltpu.VMEM((FC, out), bf16),
            pltpu.VMEM((1, out), f32),
            pltpu.VMEM((nb, nbr), i32),
            pltpu.VMEM((nb, nbr), i32),
            pltpu.VMEM((nb // GROUP, GROUP * slot), i32),
            pltpu.VMEM((nb // GROUP, GROUP * slot), i32),
            pltpu.VMEM((nb // GROUP, GROUP * slot), f32),
            pltpu.VMEM((2 * nb, D * R), bf16),
            pltpu.VMEM((D * R, FC), bf16),
            pltpu.VMEM((2 * nb, FC), f32),
            pltpu.VMEM((H, nb, share), f32),
            pltpu.VMEM((H, nb, share), f32),
            pltpu.VMEM((H - 1, nb, share), bf16),
            pltpu.VMEM((H - 1, nb, share), bf16),
            pltpu.VMEM((GROUP, nb), f32),
            pltpu.VMEM((F - 1, GROUP, nb), f32),
            dma((7,)),
            dma((lines,)), dma((lines,)), dma((lines,)), dma((lines,)),
            dma(((2 * Z - 1) * PARTS,)), dma(((2 * Z - 1) * PARTS,)),
            dma((H,)), dma((H,)), dma((H - 1,)), dma((H - 1,)), dma((F - 1,)), dma((F - 1,)),
        ],
        compiler_params=pltpu.CompilerParams(collective_id=0, has_side_effects=True),
    )(items, self_ids.reshape(1, nb), neighbor_ids.T, visit_counts.T, w_self, w_neighbor, bias.reshape(1, out))


def solution(mesh):
    placed = (
        P("dom", "feat"),
        P("dom"),
        P("dom", None),
        P("dom", None),
        P("feat", None),
        P("feat", None),
        P(),
    )
    return jax.shard_map(
        functools.partial(shards, mesh.shape["dom"], mesh.shape["feat"]),
        mesh=mesh, in_specs=placed, out_specs=P("dom", "feat"), check_vma=False,
    )
```

```python
import functools

import jax
import jax.numpy as jnp
from jax import lax
from jax.experimental import pallas as pl
from jax.experimental.pallas import tpu as pltpu
from jax.sharding import PartitionSpec as P

MESH = pl.DeviceIdType.MESH
LANES = 128
GROUP = 8
PARTS = 4


def kernel(
    D, F,
    items_hbm, self_hbm, ids_hbm, cnt_hbm, ws_hbm, wn_hbm, bias_hbm,
    out_ref,
    items, selfs, ids_t, cnt_t, ws, wn, bias,
    ids, cnt, key_s, lo_s, wgt_s, weights, gathered, acc,
    send_a, recv_a, send_b, recv_b, sq_out, sq_in,
    local_sem,
    up_send, up_recv, down_send, down_recv, x_send, x_recv,
    a_send_sem, a_recv_sem, b_send_sem, b_recv_sem, q_send_sem, q_recv_sem,
):
    dom, feat = lax.axis_index("dom"), lax.axis_index("feat")
    Z, H = D // 2, F // 2
    z, x = dom // 2, lax.rem(dom, 2)
    y, c = feat // 2, lax.rem(feat, 2)
    R, FC = items.shape
    nb = selfs.shape[1]
    nbr = ids.shape[1]
    share = out_ref.shape[1]
    slot = key_s.shape[1] // GROUP
    n_hi = D * R // LANES
    part = R // PARTS

    pairs = ((items_hbm, items), (ids_hbm, ids_t), (cnt_hbm, cnt_t), (self_hbm, selfs), (ws_hbm, ws), (wn_hbm, wn), (bias_hbm, bias))
    local = [pltpu.make_async_copy(a, b, local_sem.at[i]) for i, (a, b) in enumerate(pairs)]
    for copy in local:
        copy.start()

    barrier = pltpu.get_barrier_semaphore()

    def greet(d, f):
        pl.semaphore_signal(barrier, inc=1, device_id=(d, f), device_id_type=MESH)

    greet(dom + 1 - 2 * x, feat)

    @pl.when(z > 0)
    def _():
        greet(dom - 2, feat)

    @pl.when(z < Z - 1)
    def _():
        greet(dom + 2, feat)

    for k in range(1, F):
        greet(dom, lax.rem(feat + k, F))

    pl.semaphore_wait(barrier, F + (z > 0).astype(jnp.int32) + (z < Z - 1).astype(jnp.int32))
    local[0].wait()

    def rows_of(block, h):
        return pl.ds(pl.multiple_of(block * R + h * part, part), part)

    def block_copy(block, h, own, send_sem, recv_sem, target):
        dst = gathered.at[rows_of(block, h), :]
        src = items.at[pl.ds(h * part, part), :] if own else dst
        return pltpu.make_async_remote_copy(
            src_ref=src, dst_ref=dst, send_sem=send_sem, recv_sem=recv_sem,
            device_id=(target, feat), device_id_type=MESH,
        )

    def up_copy(s, h):
        i = s * PARTS + h
        return block_copy(dom - 2 * s, h, s == 0, up_send.at[i], up_recv.at[i], dom + 2)

    def down_copy(s, h):
        i = s * PARTS + h
        return block_copy(dom + 2 * s, h, s == 0, down_send.at[i], down_recv.at[i], dom - 2)

    def x_copy(step, h):
        i = (step + Z - 1) * PARTS + h
        return block_copy(dom + 2 * step, h, step == 0, x_send.at[i], x_recv.at[i], dom + 1 - 2 * x)

    def up_arrived(s, h):
        i = s * PARTS + h
        block_copy(dom - 2 * (s + 1), h, False, up_send.at[i], up_recv.at[i], dom).wait_recv()

    def down_arrived(s, h):
        i = s * PARTS + h
        block_copy(dom + 2 * (s + 1), h, False, down_send.at[i], down_recv.at[i], dom).wait_recv()

    def x_arrived(step, h):
        i = (step + Z - 1) * PARTS + h
        block_copy(dom + 1 - 2 * x + 2 * step, h, False, x_send.at[i], x_recv.at[i], dom).wait_recv()

    for h in range(PARTS):
        @pl.when(z < Z - 1)
        def _():
            up_copy(0, h).start()

        @pl.when(z > 0)
        def _():
            down_copy(0, h).start()

        x_copy(0, h).start()

    def forward(s, h):
        @pl.when(z > s)
        def _():
            up_arrived(s, h)

            @pl.when(z < Z - 1)
            def _():
                up_copy(s + 1, h).start()

            x_copy(-(s + 1), h).start()

        @pl.when(z < Z - 1 - s)
        def _():
            down_arrived(s, h)

            @pl.when(z > 0)
            def _():
                down_copy(s + 1, h).start()

            x_copy(s + 1, h).start()

    for copy in local[1:4]:
        copy.wait()
    ids[...] = jnp.transpose(ids_t[...])
    cnt[...] = jnp.transpose(cnt_t[...])
    wgt_s[...] = jnp.zeros_like(wgt_s)
    lo_s[...] = jnp.zeros_like(lo_s)
    key_s[...] = jnp.zeros_like(key_s)
    for j in range(GROUP):
        ids_j = ids[pl.ds(j, nb // GROUP, stride=GROUP), :]
        at = slice(j * slot, j * slot + nbr)
        key_s[:, at] = (ids_j // LANES) * GROUP + j
        lo_s[:, at] = lax.rem(ids_j, LANES)
        wgt_s[:, at] = cnt[pl.ds(j, nb // GROUP, stride=GROUP), :].astype(jnp.float32)

    K = key_s.shape[1]

    def half_group(g):
        key = key_s[pl.ds(g, 1), :]
        low = lo_s[pl.ds(g, 1), :]
        wgt = wgt_s[pl.ds(g, 1), :]
        left = jnp.where(lax.broadcasted_iota(jnp.int32, (n_hi * GROUP, K), 0) == key, wgt, 0.0)
        right = jnp.where(lax.broadcasted_iota(jnp.int32, (LANES, K), 0) == low, 1.0, 0.0)
        return lax.dot_general(
            left.astype(jnp.bfloat16), right.astype(jnp.bfloat16),
            (((1,), (1,)), ((), ())), preferred_element_type=jnp.float32,
        )

    def build(it, carry):
        first, second = half_group(it * 2), half_group(it * 2 + 1)
        at = pl.ds(pl.multiple_of(nb + it * 2 * GROUP, 2 * GROUP), 2 * GROUP)
        for hi in range(n_hi):
            rows = slice(hi * GROUP, (hi + 1) * GROUP)
            tile = jnp.concatenate([first[rows], second[rows]], axis=0)
            weights[at, hi * LANES:(hi + 1) * LANES] = tile.astype(jnp.bfloat16)
        return carry

    def build_pair(it, carry):
        return build(it * 2 + 1, build(it * 2, carry))

    pairs_here = nb // (4 * GROUP)
    for h in range(PARTS):
        lax.fori_loop(pairs_here * h // PARTS, pairs_here * (h + 1) // PARTS, build_pair, 0)
        forward(0, h)
    self_col = jnp.transpose(jnp.broadcast_to(selfs[...], (LANES, nb)))
    lane = lax.broadcasted_iota(jnp.int32, (nb, LANES), 1)
    for hi in range(n_hi):
        hit = jnp.where(self_col == lane + hi * LANES, 1.0, 0.0)
        weights[0:nb, hi * LANES:(hi + 1) * LANES] = hit.astype(jnp.bfloat16)
    total = jnp.sum(cnt[...].astype(jnp.float32), axis=1, keepdims=True)

    def columns(block):
        return weights[:, pl.ds(pl.multiple_of(block * R, R), R)]

    def add(block):
        rows = pl.ds(pl.multiple_of(block * R, R), R)
        acc[...] += jnp.dot(columns(block), gathered[rows, :], preferred_element_type=jnp.float32)

    def add_line(step, z_now, wait):
        @pl.when((z_now + step >= 0) & (z_now + step < Z))
        def _():
            if wait:
                for h in range(PARTS):
                    x_arrived(step, h)
                add(dom + 1 - 2 * x + 2 * step)
            else:
                add(dom + 2 * step)

    acc[...] = jnp.dot(columns(dom), items[...], preferred_element_type=jnp.float32)
    add_line(0, z, True)
    for s in range(Z - 1):
        if s > 0:
            for h in range(PARTS):
                forward(s, h)
        for step in (-(s + 1), s + 1):
            add_line(step, z, False)
        if s > 0:
            for step in (-s, s):
                add_line(step, z, True)
    for step in (-(Z - 1), Z - 1):
        add_line(step, z, True)

    own = acc[0:nb, :].astype(jnp.bfloat16)
    pooled = (acc[nb:2 * nb, :] / total).astype(jnp.bfloat16)
    local[4].wait()
    local[5].wait()
    local[6].wait()

    def project(yy, cc):
        cols = pl.ds(pl.multiple_of((yy * 2 + cc) * share, share), share)
        return jnp.dot(own, ws[:, cols], preferred_element_type=jnp.float32) + jnp.dot(
            pooled, wn[:, cols], preferred_element_type=jnp.float32
        )

    def a_copy(k):
        return pltpu.make_async_remote_copy(
            src_ref=send_a.at[k], dst_ref=recv_a.at[k], send_sem=a_send_sem.at[k], recv_sem=a_recv_sem.at[k],
            device_id=(dom, feat + 1 - 2 * c), device_id_type=MESH,
        )

    def b_copy(k):
        return pltpu.make_async_remote_copy(
            src_ref=send_b.at[k], dst_ref=recv_b.at[k], send_sem=b_send_sem.at[k], recv_sem=b_recv_sem.at[k],
            device_id=(dom, lax.rem(y + k + 1, H) * 2 + c), device_id_type=MESH,
        )

    for k in range(H):
        send_a[k] = project(lax.rem(y + k + 1, H), 1 - c)
        a_copy(k).start()
    mine = None
    for k in range(H):
        here = project(lax.rem(y + k + 1, H), c)
        a_copy(k).wait_recv()
        summed = here + recv_a[k]
        if k < H - 1:
            send_b[k] = summed.astype(jnp.bfloat16)
            b_copy(k).start()
        else:
            mine = summed + bias[:, pl.ds(pl.multiple_of(feat * share, share), share)]
    for k in range(H - 1):
        b_copy(k).wait_recv()
        mine = mine + recv_b[k].astype(jnp.float32)
    hidden = jnp.maximum(mine, 0.0)
    squares = jnp.sum(hidden * hidden, axis=1, keepdims=True)
    row = jnp.transpose(jnp.broadcast_to(squares, (nb, LANES)))[0:GROUP, :]
    sq_out[...] = row

    def q_copy(k):
        return pltpu.make_async_remote_copy(
            src_ref=sq_out, dst_ref=sq_in.at[k - 1], send_sem=q_send_sem.at[k - 1], recv_sem=q_recv_sem.at[k - 1],
            device_id=(dom, lax.rem(feat + k, F)), device_id_type=MESH,
        )

    for k in range(1, F):
        q_copy(k).start()
    for k in range(1, F):
        q_copy(k).wait_recv()
        row = row + sq_in[k - 1]
    scale = lax.rsqrt(row / (share * F) + 1e-06)[0:1, :]
    column = jnp.transpose(jnp.broadcast_to(scale, (LANES, nb)))
    for i in range(share // LANES):
        at = slice(i * LANES, (i + 1) * LANES)
        out_ref[:, at] = hidden[:, at] * column

    for s in range(Z - 1):
        for h in range(PARTS):
            @pl.when((z < Z - 1) & (z >= s))
            def _():
                up_copy(s, h).wait_send()

            @pl.when((z > 0) & (z < Z - s))
            def _():
                down_copy(s, h).wait_send()
    for step in range(-(Z - 1), Z):
        @pl.when((z + step >= 0) & (z + step < Z))
        def _():
            for h in range(PARTS):
                x_copy(step, h).wait_send()
    for k in range(H):
        a_copy(k).wait_send()
    for k in range(H - 1):
        b_copy(k).wait_send()
    for k in range(1, F):
        q_copy(k).wait_send()


def shards(D, F, items, self_ids, neighbor_ids, visit_counts, w_self, w_neighbor, bias):
    R, FC = items.shape
    nb, nbr = neighbor_ids.shape
    out = bias.shape[0]
    share = out // F
    slot = 1 << (nbr - 1).bit_length()
    Z, H = D // 2, F // 2
    lines = (Z - 1) * PARTS
    f32, bf16, i32 = jnp.float32, jnp.bfloat16, jnp.int32
    dma = pltpu.SemaphoreType.DMA
    return pl.pallas_call(
        functools.partial(kernel, D, F),
        out_shape=pltpu.VMEM((nb, share), f32),
        in_specs=[pl.BlockSpec(memory_space=pl.ANY)] * 7,
        out_specs=pl.BlockSpec(memory_space=pltpu.VMEM),
        scratch_shapes=[
            pltpu.VMEM((R, FC), bf16),
            pltpu.VMEM((1, nb), i32),
            pltpu.VMEM((nbr, nb), i32),
            pltpu.VMEM((nbr, nb), i32),
            pltpu.VMEM((FC, out), bf16),
            pltpu.VMEM((FC, out), bf16),
            pltpu.VMEM((1, out), f32),
            pltpu.VMEM((nb, nbr), i32),
            pltpu.VMEM((nb, nbr), i32),
            pltpu.VMEM((nb // GROUP, GROUP * slot), i32),
            pltpu.VMEM((nb // GROUP, GROUP * slot), i32),
            pltpu.VMEM((nb // GROUP, GROUP * slot), f32),
            pltpu.VMEM((2 * nb, D * R), bf16),
            pltpu.VMEM((D * R, FC), bf16),
            pltpu.VMEM((2 * nb, FC), f32),
            pltpu.VMEM((H, nb, share), f32),
            pltpu.VMEM((H, nb, share), f32),
            pltpu.VMEM((H - 1, nb, share), bf16),
            pltpu.VMEM((H - 1, nb, share), bf16),
            pltpu.VMEM((GROUP, nb), f32),
            pltpu.VMEM((F - 1, GROUP, nb), f32),
            dma((7,)),
            dma((lines,)), dma((lines,)), dma((lines,)), dma((lines,)),
            dma(((2 * Z - 1) * PARTS,)), dma(((2 * Z - 1) * PARTS,)),
            dma((H,)), dma((H,)), dma((H - 1,)), dma((H - 1,)), dma((F - 1,)), dma((F - 1,)),
        ],
        compiler_params=pltpu.CompilerParams(collective_id=0, has_side_effects=True),
    )(items, self_ids.reshape(1, nb), neighbor_ids.T, visit_counts.T, w_self, w_neighbor, bias.reshape(1, out))


def solution(mesh):
    placed = (
        P("dom", "feat"),
        P("dom"),
        P("dom", None),
        P("dom", None),
        P("feat", None),
        P("feat", None),
        P(),
    )
    return jax.shard_map(
        functools.partial(shards, mesh.shape["dom"], mesh.shape["feat"]),
        mesh=mesh, in_specs=placed, out_specs=P("dom", "feat"), check_vma=False,
    )
```
